32 devices in a mesh: outer: 4 (over y, x), inner: 8 (over z, core).
Axes of the slice: x: 2, y: 2, z: 4, core: 2. Of those that a mesh axis runs over, the one named last changes fastest.
Arguments:
- tokens: bfloat16 [4096, 4096], P('inner', 'outer'), may hold values from -6 to 6
- cotangent: bfloat16 [4096, 4096], P('inner', 'outer'), may hold values from -0.09375 to 0.09375
- weight_cache: bfloat16 [4096, 4096], P(None, 'outer'), may hold values from -0.09375 to 0.09375
- weight_delta: bfloat16 [4096, 4096], P('inner', 'outer'), may hold values from -0.078125 to 0.078125
- sign_bits: int32 [4096], P('outer'), may hold values from 0 to 1
- master: float32 [4096, 4096], P('inner', 'outer'), may hold values from -1.5 to 1.5
- moment: float32 [4096, 4096], P('inner', 'outer'), may hold values from -6 to 6
- variance: float32 [4096, 4096], P('inner', 'outer'), may hold values from 0.25 to 4
Outputs:
- activation: float32 [4096, 4096], P('inner', 'outer')
- new_master: float32 [4096, 4096], P('inner', 'outer')
- new_moment: float32 [4096, 4096], P('inner', 'outer')
- new_variance: float32 [4096, 4096], P('inner', 'outer')
- block_scales: float32 [4096, 32], P('inner', 'outer')
The draws below stay inside these ranges and needn't reach their ends.
All inputs are finite; a program needn't handle non-finite values.
Results may differ from the reference program's by a relative error of at most 0.003.
Values may be sent and summed in bfloat16 or wider, within the bound.
No kernel may reach another device: no remote copies, remote signals or barrier semaphores. Data moves between devices by JAX's collectives and lax.ppermute only.
A program may use at most 128 MiB of HBM per device.

```python
import math
import jax
import jax.numpy as jnp
from jax import lax

IN_FEAT = 4096
OUT_FEAT = 4096
BLOCK = 128
TOKENS = 4096


def place_ends(result, key, least, largest):
    longest = result.shape.index(max(result.shape))
    spots = []
    for shift in (0, 1):
        where = [jax.random.randint(jax.random.fold_in(key, axis), (), 0, length) for axis, length in enumerate(result.shape)]
        where[longest] = (where[longest] + shift) % result.shape[longest]
        spots.append(tuple(where))
    return result.at[spots[0]].set(least).at[spots[1]].set(largest)


def spiked(drawn, stream_key, source, target, blocks, factor):
    def block_of(position):
        return (jnp.arange(drawn.shape[position]) // (drawn.shape[position] // blocks)).reshape((-1,) + (1,) * (drawn.ndim - 1 - position))

    near = jax.random.permutation(stream_key, blocks)[block_of(target)]
    other_side = (block_of(target) + blocks // 2) % blocks
    return jnp.where((block_of(source) == near) | (block_of(source) == other_side), factor * drawn, drawn)


def shard_levels(stream_key, dims, pieces, smallest, high):
    level, own = 1.0, jax.random.fold_in(stream_key, 6)
    for dim, parts in pieces:
        heights = jnp.exp(jax.random.uniform(jax.random.fold_in(own, dim), (parts,), jnp.float32, smallest / len(pieces), high / len(pieces)))
        level = level * jnp.repeat(heights, dims[dim] // parts).reshape([-1 if axis == dim else 1 for axis in range(len(dims))])
    return level


def scatter_about(key, extent, scale, reach, shards=(), kind=jnp.bfloat16):
    array = jax.random.normal(key, extent, jnp.float32) * scale
    if len(shards) > 0:
        array = shard_levels(key, extent, shards, -0.22, 0.18) * array
    return jnp.clip(array, min=-reach, max=reach).astype(kind)


def heavy_noise(key, shape, width, reach, split, heavy, held_as=jnp.bfloat16):
    result = width * jax.random.normal(key, shape, jnp.float32)
    if split:
        result = result * shard_levels(key, shape, split, -0.22, 0.18)
    return jnp.clip(spiked(result, jax.random.fold_in(key, 3), *heavy), -reach, reach).astype(held_as)


def setup_inputs(seed: int = 0) -> dict:
    arg_keys = jax.random.split(jax.random.key(seed), 9)
    return {
        "tokens": heavy_noise(arg_keys[0], (TOKENS, IN_FEAT), 1.0, 6.0, ((0, 8), (1, 4)), (0, 1, 8, 2.0)),
        "cotangent": scatter_about(arg_keys[1], (TOKENS, OUT_FEAT), TOKENS ** -0.5, 0.09375, ((0, 8), (1, 4))),
        "weight_cache": scatter_about(arg_keys[2], (IN_FEAT, OUT_FEAT), IN_FEAT ** -0.5, 0.09375, ((1, 4),)),
        "weight_delta": scatter_about(arg_keys[3], (IN_FEAT, OUT_FEAT), 0.005, 0.078125, ((0, 8), (1, 4))),
        "sign_bits": place_ends(jax.random.randint(arg_keys[4], (OUT_FEAT,), 0, 2), jax.random.fold_in(arg_keys[4], 1), 0, 1).astype(jnp.int32),
        "master": scatter_about(arg_keys[5], (IN_FEAT, OUT_FEAT), 0.1, 1.5, ((0, 8), (1, 4)), jnp.float32),
        "moment": scatter_about(arg_keys[6], (IN_FEAT, OUT_FEAT), 0.5, 6.0, ((0, 8), (1, 4)), jnp.float32),
        "variance": jnp.clip(jnp.exp(math.log(4.0) - 2.7725887 * jax.random.uniform(arg_keys[7], (IN_FEAT, OUT_FEAT), jnp.float32) ** shard_levels(arg_keys[7], (IN_FEAT, OUT_FEAT), ((0, 8), (1, 4)), -0.2, 0.2)), 0.25, 4.0),
    }


def hadamard_table(length):
    first = jnp.arange(length, dtype=jnp.int32)[:, None]
    second = jnp.arange(length, dtype=jnp.int32)[None, :]
    common = jnp.bitwise_and(first, second)
    parity = jnp.zeros((length, length), jnp.int32)
    for place in range(length.bit_length() - 1):
        parity = parity + jnp.bitwise_and(jnp.right_shift(common, place), 1)
    return (1 - 2 * (parity % 2)).astype(jnp.float32) / jnp.sqrt(jnp.float32(length))

def smooth(values, signs, table):
    height = values.shape[0]
    blocks = values.reshape(height, -1, table.shape[0]) * signs.reshape(-1, table.shape[0])
    mixed = jnp.einsum('rbk,kj->rbj', blocks, table, precision=lax.Precision.HIGHEST)
    return mixed.reshape(height, -1)

def unsmooth(values, signs, table):
    height = values.shape[0]
    blocks = values.reshape(height, -1, table.shape[0])
    mixed = jnp.einsum('rbj,jk->rbk', blocks, table, precision=lax.Precision.HIGHEST)
    return (mixed * signs.reshape(-1, table.shape[0])).reshape(height, -1)

def reference(tokens, cotangent, weight_cache, weight_delta, sign_bits, master, moment, variance):
    weight = (weight_cache.astype(jnp.float32) + weight_delta.astype(jnp.float32)).astype(jnp.bfloat16)
    activation = jnp.dot(tokens, weight, preferred_element_type=jnp.float32)
    gradient = lax.dot_general(tokens, cotangent, (((0,), (0,)), ((), ())), preferred_element_type=jnp.float32)
    table = hadamard_table(BLOCK)
    signs = (1 - 2 * sign_bits).astype(jnp.float32)
    smoothed = smooth(gradient, signs, table)
    block_scales = lax.optimization_barrier(jnp.max(jnp.abs(smoothed.reshape(IN_FEAT, -1, BLOCK)), axis=2))
    restored = unsmooth(smoothed, signs, table)
    new_moment = 0.9 * moment + 0.1 * restored
    new_variance = 0.95 * variance + 0.05 * restored * restored
    corrected = new_moment / (1.0 - 0.9 ** 10)
    spread = jnp.sqrt(new_variance / (1.0 - 0.95 ** 10)) + 1e-08
    new_master = master - 0.01 * (corrected / spread + 0.1 * master)
    return (activation, new_master, new_moment, new_variance, block_scales)
```

```python
import functools

import jax
import jax.numpy as jnp
from jax import lax
from jax.experimental import pallas as pl
from jax.experimental.pallas import tpu as pltpu
from jax.sharding import PartitionSpec as P

BLOCK = 128
PARTS = 2


def sign_table(length):
    first = jnp.arange(length, dtype=jnp.int32)[:, None]
    second = jnp.arange(length, dtype=jnp.int32)[None, :]
    common = jnp.bitwise_and(first, second)
    parity = jnp.zeros((length, length), jnp.int32)
    for place in range(length.bit_length() - 1):
        parity = parity + jnp.bitwise_and(jnp.right_shift(common, place), 1)
    return 1 - 2 * (parity % 2)


def finish_kernel(signs, table, own, ours, theirs, master, moment, variance, *rest):
    new_master, new_moment, new_variance, scales = rest[-4:]
    gradient = own[...] + ours[...].astype(jnp.float32) + theirs[...].astype(jnp.float32)
    first = 0.9 * moment[...] + 0.1 * gradient
    second = 0.95 * variance[...] + 0.05 * gradient * gradient
    corrected = first / (1.0 - 0.9**10)
    spread = jnp.sqrt(second / (1.0 - 0.95**10)) + 1e-08
    new_moment[...] = first
    new_variance[...] = second
    new_master[...] = master[...] - 0.01 * (corrected / spread + 0.1 * master[...])
    for place in range(gradient.shape[1] // BLOCK):
        columns = slice(place * BLOCK, (place + 1) * BLOCK)
        signed = gradient[:, columns] * signs[:, columns]
        high = signed.astype(jnp.bfloat16)
        low = (signed - high.astype(jnp.float32)).astype(jnp.bfloat16)
        mixed = sum(
            lax.dot_general(
                table[...], term, (((1,), (1,)), ((), ())), preferred_element_type=jnp.float32
            )
            for term in (high, low)
        )
        largest = jnp.max(jnp.abs(mixed), axis=0, keepdims=True)
        scales[place : place + 1, :] = largest * (1.0 / BLOCK**0.5)


def finish(part, parts, signs, table, own, ours, theirs, master, moment, variance, before):
    rows, width = master.shape
    size = rows // parts
    tile = min(size, 128)
    steps = size // tile
    offset = part * steps
    whole = pl.BlockSpec((tile, width), lambda k: (k + offset, 0))
    piece = pl.BlockSpec((tile, width), lambda k: (k, 0))
    scale = pl.BlockSpec((width // BLOCK, tile), lambda k: (0, k + offset))
    given = [
        pl.BlockSpec((1, width), lambda k: (0, 0)),
        pl.BlockSpec((BLOCK, BLOCK), lambda k: (0, 0)),
        whole,
        piece,
        whole,
        whole,
        whole,
        whole,
    ]
    kept = [pl.BlockSpec(memory_space=pl.ANY)] * len(before)
    return pl.pallas_call(
        finish_kernel,
        grid=(steps,),
        in_specs=given + kept,
        out_specs=[whole, whole, whole, scale],
        out_shape=[jax.ShapeDtypeStruct(master.shape, jnp.float32)] * 3
        + [jax.ShapeDtypeStruct((width // BLOCK, rows), jnp.float32)],
        input_output_aliases={len(given) + k: k for k in range(len(before))},
        name=f"finish_{part}",
    )(signs, table, own, ours, theirs, master, moment, variance, *before)


def gather_tokens(low, high, outer):
    if outer != 4:
        lows = lax.all_gather(low, "outer", axis=0, tiled=False)
        highs = lax.all_gather(high, "outer", axis=0, tiled=False)
        return [(lows[k], 0, k) for k in range(outer)] + [(highs[k], 1, k) for k in range(outer)]
    me = lax.axis_index("outer")
    even = (me == 0) | (me == 3)

    def across(value, distance):
        return lax.ppermute(value, "outer", [(k, k ^ distance) for k in range(outer)])

    near, far, corner = me ^ 1, me ^ 2, me ^ 3
    near_low = across(low, 1)
    far_high = across(high, 2)
    second_near = across(jnp.where(even, high, far_high), 1)
    second_far = across(jnp.where(even, low, near_low), 2)
    third_near = across(jnp.where(even, far_high, high), 1)
    third_far = across(jnp.where(even, near_low, low), 2)
    return [
        (low, 0, me),
        (high, 1, me),
        (near_low, 0, near),
        (far_high, 1, far),
        (second_near, 1, jnp.where(even, corner, near)),
        (second_far, 0, jnp.where(even, corner, far)),
        (third_near, 1, jnp.where(even, near, corner)),
        (third_far, 0, jnp.where(even, far, corner)),
    ]


def make_body(outer, inner):
    chips = inner // 2
    swap_pairs = [(k, k ^ 1) for k in range(inner)]
    up = [[(2 * z + c, 2 * z + 2 + c) for z in range(chips - 1)] for c in (0, 1)]
    down = [[(2 * z + c, 2 * z - 2 + c) for z in range(1, chips)] for c in (0, 1)]
    line_pairs = (up[0] + down[1], up[1] + down[0])

    def swap(value):
        return lax.ppermute(value, "inner", swap_pairs)

    def body(tokens, cotangent, weight_cache, weight_delta, sign_bits, master, moment, variance):
        index = lax.axis_index("inner")
        chip, core = index // 2, index % 2
        rows, width = master.shape
        count, wide = tokens.shape
        group = wide // (2 * rows)
        signs = (1 - 2 * sign_bits).astype(jnp.float32)[None, :]
        table = sign_table(BLOCK).astype(jnp.bfloat16)
        upward = (core == 0, core == 1)

        def turned(line, position):
            return jnp.where(upward[line], position, chips - 1 - position)

        places = [turned(line, chip) for line in (0, 1)]

        def columns_of(core_index):
            grouped = tokens.reshape(count, group, 2, rows)
            return lax.dynamic_index_in_dim(grouped, core_index, 2, keepdims=False).reshape(
                count, group * rows
            )

        low = columns_of(core)
        high = swap(columns_of(1 - core))
        cotangents = jnp.concatenate([cotangent, swap(cotangent)], axis=0)
        held = jnp.zeros((outer, 2 * count, wide // 2), tokens.dtype)
        for piece, which, owner in gather_tokens(low, high, outer):
            held = lax.dynamic_update_slice(held, piece[None], (owner, which * count, 0))

        def tokens_for(chip_index):
            return lax.dynamic_slice(
                held,
                (chip_index // group, 0, lax.rem(chip_index, group) * rows),
                (1, 2 * count, rows),
            )[0]

        def partial_sum(chip_index):
            return lax.dot_general(
                tokens_for(chip_index),
                cotangents,
                (((0,), (0,)), ((), ())),
                preferred_element_type=jnp.float32,
            )

        def product(chip_index, delta):
            cached = lax.dynamic_slice(
                weight_cache, ((2 * chip_index + core) * rows, 0), (rows, width)
            )
            weight = (cached.astype(jnp.float32) + delta.astype(jnp.float32)).astype(jnp.bfloat16)
            return jnp.dot(tokens_for(chip_index), weight, preferred_element_type=jnp.float32)

        message = [weight_delta, weight_delta]
        history = ([], [])
        own = partial_sum(chip)
        for turn in range(1, chips):
            for line in (0, 1):
                received = lax.ppermute(message[line], "inner", line_pairs[line])
                history[line].append(received)
                place = places[line]
                target = turned(line, lax.rem(place - turn + chips, chips))
                term = jnp.where(turn <= place, jnp.float32(0), partial_sum(target))
                message[line] = (received.astype(jnp.float32) + term).astype(jnp.bfloat16)

        first = lax.ppermute(message[0], "inner", line_pairs[0])
        parts = max(1, min(PARTS, rows // 128))
        size = rows // parts
        second = [
            lax.ppermute(message[1][k * size : (k + 1) * size], "inner", line_pairs[1])
            for k in range(parts)
        ]

        both = product(chip, weight_delta)
        for turn in sorted(range(1, chips), key=lambda t: max(t, chips - t)):
            delta = jnp.where(
                turn <= places[0], history[0][turn - 1], history[1][chips - turn - 1]
            )
            source = turned(0, lax.rem(places[0] - turn + chips, chips))
            both = both + product(source, delta)
        output = both[:count] + swap(both[count:])

        done = []
        for k in range(parts):
            done = finish(
                k, parts, signs, table, own, second[k], first, master, moment, variance, done
            )
        new_master, new_moment, new_variance, scales = done
        return (output, new_master, new_moment, new_variance, scales.T)

    return body


def solution(mesh):
    placed = (
        P("inner", "outer"),
        P("inner", "outer"),
        P(None, "outer"),
        P("inner", "outer"),
        P("outer"),
        P("inner", "outer"),
        P("inner", "outer"),
        P("inner", "outer"),
    )
    return jax.shard_map(
        make_body(mesh.shape["outer"], mesh.shape["inner"]),
        mesh=mesh,
        in_specs=placed,
        out_specs=(
            P("inner", "outer"),
            P("inner", "outer"),
            P("inner", "outer"),
            P("inner", "outer"),
            P("inner", "outer"),
        ),
        check_vma=False,
    )
```

```python
import jax
import jax.numpy as jnp
from jax import lax
from jax.experimental import pallas as pl
from jax.sharding import PartitionSpec as P


BLOCK = 128
PARTS = 2


def sign_table(length):
    first = jnp.arange(length, dtype=jnp.int32)[:, None]
    second = jnp.arange(length, dtype=jnp.int32)[None, :]
    common = jnp.bitwise_and(first, second)
    parity = jnp.zeros((length, length), jnp.int32)
    for place in range(length.bit_length() - 1):
        parity = parity + jnp.bitwise_and(jnp.right_shift(common, place), 1)
    return 1 - 2 * (parity % 2)


def finish_kernel(signs, table, kept, own, first, second, master, moment, variance, *rest):
    new_master, new_moment, new_variance, scales = rest[-4:]
    step = pl.program_id(0)
    gradient = own[...]
    for line, received in enumerate((first, second)):
        wanted = kept[:, line : line + 1] > 0.0
        gradient = gradient + jnp.where(wanted, received[...].astype(jnp.float32), 0.0)
    first = 0.9 * moment[...] + 0.1 * gradient
    second = 0.95 * variance[...] + 0.05 * gradient * gradient
    corrected = first / (1.0 - 0.9**10)
    spread = jnp.sqrt(second / (1.0 - 0.95**10)) + 1e-08
    new_moment[...] = first
    new_variance[...] = second
    new_master[...] = master[...] - 0.01 * (corrected / spread + 0.1 * master[...])
    for place in range(gradient.shape[1] // BLOCK):
        columns = slice(place * BLOCK, (place + 1) * BLOCK)
        signed = gradient[:, columns] * signs[:, columns]
        high = signed.astype(jnp.bfloat16)
        low = (signed - high.astype(jnp.float32)).astype(jnp.bfloat16)
        mixed = sum(
            lax.dot_general(
                table[...], term, (((1,), (1,)), ((), ())), preferred_element_type=jnp.float32
            )
            for term in (high, low)
        )
        largest = jnp.max(jnp.abs(mixed), axis=0, keepdims=True)
        row = step * (gradient.shape[1] // BLOCK) + place
        scales[pl.ds(row, 1), :] = largest * (1.0 / BLOCK**0.5)


def finish(
    part, parts, signs, table, kept, own, first, second, master, moment, variance, before
):
    rows, width = master.shape
    size = rows // parts
    tile = min(width, 512)
    whole = pl.BlockSpec((size, tile), lambda k: (part, k))
    piece = pl.BlockSpec((size, tile), lambda k: (0, k))
    given = [
        pl.BlockSpec((1, tile), lambda k: (0, k)),
        pl.BlockSpec((BLOCK, BLOCK), lambda k: (0, 0)),
        pl.BlockSpec((1, 2), lambda k: (0, 0)),
        whole,
        piece,
        piece,
        whole,
        whole,
        whole,
    ]
    held = [pl.BlockSpec(memory_space=pl.ANY)] * len(before)
    return pl.pallas_call(
        finish_kernel,
        grid=(width // tile,),
        in_specs=given + held,
        out_specs=[
            whole,
            whole,
            whole,
            pl.BlockSpec((width // BLOCK, size), lambda k: (0, part)),
        ],
        out_shape=[jax.ShapeDtypeStruct(master.shape, jnp.float32)] * 3
        + [jax.ShapeDtypeStruct((width // BLOCK, rows), jnp.float32)],
        input_output_aliases={len(given) + k: k for k in range(len(before))},
    )(signs, table, kept, own, first, second, master, moment, variance, *before)


def gather_tokens(lows, highs, outer):
    parts = len(lows)
    if outer != 4:
        every = []
        for which, pieces in enumerate((lows, highs)):
            for part, piece in enumerate(pieces):
                whole = lax.all_gather(piece, "outer", axis=0, tiled=False)
                every += [(whole[k], which, part, k) for k in range(outer)]
        return every, None
    me = lax.axis_index("outer")
    even = (me == 0) | (me == 3)

    def across(value, distance):
        return lax.ppermute(value, "outer", [(k, k ^ distance) for k in range(outer)])

    near, far, corner = me ^ 1, me ^ 2, me ^ 3
    near_low = [across(lows[k], 1) for k in range(parts)]
    far_high = [across(highs[k], 2) for k in range(parts)]
    second_near = [across(jnp.where(even, highs[k], far_high[k]), 1) for k in range(parts)]
    second_far = [across(jnp.where(even, lows[k], near_low[k]), 2) for k in range(parts)]
    all_of = [jnp.concatenate(pieces, axis=1) for pieces in (lows, highs, near_low, far_high)]
    third_near = across(jnp.where(even, all_of[3], all_of[1]), 1)
    third_far = across(jnp.where(even, all_of[2], all_of[0]), 2)

    def end_block(owner, part):
        one = jnp.where(
            owner == me,
            lows[part],
            jnp.where(owner == near, near_low[part], second_far[part]),
        )
        two = jnp.where(
            owner == me,
            highs[part],
            jnp.where(owner == far, far_high[part], second_near[part]),
        )
        return one, two

    every = []
    for k in range(parts):
        every += [
            (lows[k], 0, k, me),
            (highs[k], 1, k, me),
            (near_low[k], 0, k, near),
            (far_high[k], 1, k, far),
            (second_near[k], 1, k, jnp.where(even, corner, near)),
            (second_far[k], 0, k, jnp.where(even, corner, far)),
        ]
    every += [
        (third_near, 1, 0, jnp.where(even, near, corner)),
        (third_far, 0, 0, jnp.where(even, far, corner)),
    ]
    return every, end_block


def contract(left, right):
    return lax.dot_general(
        left, right, (((0,), (0,)), ((), ())), preferred_element_type=jnp.float32
    )


def make_body(outer, inner):
    chips = inner // 2
    swap_pairs = [(k, k ^ 1) for k in range(inner)]
    up, down = [], []
    for z in range(chips - 1):
        up.append([(2 * z, 2 * z + 2), (2 * z + 1, 2 * z + 3)])
        down.append([(2 * z + 2, 2 * z), (2 * z + 3, 2 * z + 1)])
    top = 2 * chips - 2
    line_pairs = (
        [pair[0] for pair in up] + [pair[1] for pair in down] + [(top, top + 1), (1, 0)],
        [pair[1] for pair in up] + [pair[0] for pair in down] + [(top + 1, top), (0, 1)],
    )

    def swap(value):
        return lax.ppermute(value, "inner", swap_pairs)

    def along(line, value):
        return lax.ppermute(value, "inner", line_pairs[line])

    def body(tokens, cotangent, weight_cache, weight_delta, sign_bits, master, moment, variance):
        index = lax.axis_index("inner")
        chip, core = index // 2, index % 2
        rows, width = master.shape
        count, wide = tokens.shape
        group = wide // (2 * rows)
        signs = (1 - 2 * sign_bits).astype(jnp.float32)[None, :]
        table = sign_table(BLOCK).astype(jnp.bfloat16)
        upward = (core == 0, core == 1)

        def turned(line, position):
            return jnp.where(upward[line], position, chips - 1 - position)

        places = [turned(line, chip) for line in (0, 1)]

        parts = max(1, min(PARTS, rows // 128))
        size = rows // parts

        def columns_of(core_index, part):
            starts = [(2 * k + core_index) * rows + part * size for k in range(group)]
            return jnp.concatenate(
                [lax.dynamic_slice(tokens, (0, start), (count, size)) for start in starts],
                axis=1,
            )

        cut = [columns_of(which, part) for which in (core, 1 - core) for part in range(parts)]
        cut = lax.optimization_barrier(cut)
        lows = cut[:parts]
        highs = [swap(cut[parts + k]) for k in range(parts)]
        pieces, end_block = gather_tokens(lows, highs, outer)
        if chips != outer:
            end_block = None
        kept = [jnp.where(place == 0, 0.0, 1.0) for place in places]
        kept = jnp.stack(kept).astype(jnp.float32).reshape(1, 2)
        signs, table, kept, cotangent = lax.optimization_barrier((signs, table, kept, cotangent))
        cotangent_other = swap(cotangent)
        cotangents = jnp.concatenate([cotangent, cotangent_other], axis=0)
        held = jnp.zeros((outer, 2 * count, group, rows), tokens.dtype)
        for piece, which, part, owner in pieces:
            piece = piece.reshape(1, count, group, -1)
            held = lax.dynamic_update_slice(
                held, piece, (owner, which * count, 0, part * size)
            )
        held = held.reshape(outer, 2 * count, group * rows)

        def tokens_for(chip_index, which=None):
            first, size = (0, 2 * count) if which is None else (which * count, count)
            return lax.dynamic_slice(
                held,
                (chip_index // group, first, lax.rem(chip_index, group) * rows),
                (1, size, rows),
            )[0]

        def partial_sum(chip_index):
            return contract(tokens_for(chip_index), cotangents)

        def product(chip_index, delta, cache):
            cached = lax.dynamic_slice(cache, ((2 * chip_index + core) * rows, 0), (rows, width))
            weight = cached.astype(jnp.float32) + delta.astype(jnp.float32)
            weight = lax.optimization_barrier(weight.astype(jnp.bfloat16))
            return [
                jnp.dot(tokens_for(chip_index, which), weight, preferred_element_type=jnp.float32)
                for which in (0, 1)
            ]

        message = [[weight_delta], [weight_delta]]
        history = ([], [])
        cache = weight_cache
        caches = [cache]
        for turn in range(1, chips):
            terms = []
            for line in (0, 1):
                history[line].append([along(line, value) for value in message[line]])
                if turn > 1 or end_block is None:
                    target = turned(line, lax.rem(places[line] - turn + chips, chips))
                    term = partial_sum(target)
                    term = jnp.where(turn <= places[line], jnp.float32(0), term)
                    terms.append(lax.optimization_barrier(term))
            message = [[], []]
            for k in range(parts):
                rows_of = slice(k * size, (k + 1) * size)
                for line in (0, 1):
                    received, place = history[line][-1], places[line]
                    if terms:
                        term = terms[line][rows_of]
                    else:
                        one, two = end_block(turned(line, chips - 1), k)
                        term = contract(one, cotangent) + contract(two, cotangent_other)
                        term = jnp.where(turn <= place, jnp.float32(0), term)
                    before = received[0][rows_of] if len(received) == 1 else received[k]
                    before = jnp.where(place == 0, jnp.bfloat16(0), before)
                    value = (before.astype(jnp.float32) + term).astype(jnp.bfloat16)
                    cache, value, cotangent_other, *terms = lax.optimization_barrier(
                        (cache, value, cotangent_other, *terms)
                    )
                    message[line].append(value)
            caches.append(cache)

        last = [[along(line, message[line][k]) for line in (0, 1)] for k in range(parts)]
        own = lax.optimization_barrier(partial_sum(chip))

        mine, other = product(chip, weight_delta, caches[min(2, chips - 1)])
        order = sorted(range(1, chips), key=lambda t: max(t, chips - t))
        products = []
        for number, turn in enumerate(order, 1):
            passed = [history[0][turn - 1], history[1][chips - turn - 1]]
            most = max(len(value) for value in passed)
            for line in (0, 1):
                if len(passed[line]) < most:
                    whole = passed[line][0]
                    passed[line] = [
                        whole[k * size : (k + 1) * size] for k in range(most)
                    ]
            delta = jnp.concatenate(
                [jnp.where(turn <= places[0], one, two) for one, two in zip(*passed)], axis=0
            )
            source = turned(0, lax.rem(places[0] - turn + chips, chips))
            one, two = product(source, delta, caches[max(turn, chips - turn)])
            other = other + two
            products.append((number, one))
        theirs = swap(other)
        for number, one in products:
            mine = lax.optimization_barrier(mine)
            if number == chips - 1:
                mine = mine + theirs
            mine = mine + one
        output = mine

        done = []
        for k in range(parts):
            done = finish(
                k, parts, signs, table, kept, own, *last[k], master, moment, variance, done
            )
        new_master, new_moment, new_variance, scales = done
        return (output, new_master, new_moment, new_variance, scales.T)

    return body


def solution(mesh):
    placed = (
        P("inner", "outer"),
        P("inner", "outer"),
        P(None, "outer"),
        P("inner", "outer"),
        P("outer"),
        P("inner", "outer"),
        P("inner", "outer"),
        P("inner", "outer"),
    )
    return jax.shard_map(
        make_body(mesh.shape["outer"], mesh.shape["inner"]),
        mesh=mesh,
        in_specs=placed,
        out_specs=(
            P("inner", "outer"),
            P("inner", "outer"),
            P("inner", "outer"),
            P("inner", "outer"),
            P("inner", "outer"),
        ),
        check_vma=False,
    )
```

```python
import jax
import jax.numpy as jnp
from jax import lax
from jax.experimental import pallas as pl
from jax.sharding import PartitionSpec as P


BLOCK = 128
PARTS = 2


def sign_table(length):
    first = jnp.arange(length, dtype=jnp.int32)[:, None]
    second = jnp.arange(length, dtype=jnp.int32)[None, :]
    common = jnp.bitwise_and(first, second)
    parity = jnp.zeros((length, length), jnp.int32)
    for place in range(length.bit_length() - 1):
        parity = parity + jnp.bitwise_and(jnp.right_shift(common, place), 1)
    return 1 - 2 * (parity % 2)


def finish_kernel(signs, table, kept, own, first, second, master, moment, variance, *rest):
    new_master, new_moment, new_variance, scales = rest[-4:]
    step = pl.program_id(0)
    gradient = own[...]
    for line, received in enumerate((first, second)):
        wanted = kept[:, line : line + 1] > 0.0
        gradient = gradient + jnp.where(wanted, received[...].astype(jnp.float32), 0.0)
    first = 0.9 * moment[...] + 0.1 * gradient
    second = 0.95 * variance[...] + 0.05 * gradient * gradient
    corrected = first / (1.0 - 0.9**10)
    spread = jnp.sqrt(second / (1.0 - 0.95**10)) + 1e-08
    new_moment[...] = first
    new_variance[...] = second
    new_master[...] = master[...] - 0.01 * (corrected / spread + 0.1 * master[...])
    for place in range(gradient.shape[1] // BLOCK):
        columns = slice(place * BLOCK, (place + 1) * BLOCK)
        signed = gradient[:, columns] * signs[:, columns]
        high = signed.astype(jnp.bfloat16)
        low = (signed - high.astype(jnp.float32)).astype(jnp.bfloat16)
        mixed = sum(
            lax.dot_general(
                table[...], term, (((1,), (1,)), ((), ())), preferred_element_type=jnp.float32
            )
            for term in (high, low)
        )
        largest = jnp.max(jnp.abs(mixed), axis=0, keepdims=True)
        row = step * (gradient.shape[1] // BLOCK) + place
        scales[pl.ds(row, 1), :] = largest * (1.0 / BLOCK**0.5)


def finish(
    part, parts, signs, table, kept, own, first, second, master, moment, variance, before
):
    rows, width = master.shape
    size = rows // parts
    tile = min(width, 512)
    whole = pl.BlockSpec((size, tile), lambda k: (part, k))
    piece = pl.BlockSpec((size, tile), lambda k: (0, k))
    given = [
        pl.BlockSpec((1, tile), lambda k: (0, k)),
        pl.BlockSpec((BLOCK, BLOCK), lambda k: (0, 0)),
        pl.BlockSpec((1, 2), lambda k: (0, 0)),
        whole,
        piece,
        piece,
        whole,
        whole,
        whole,
    ]
    held = [pl.BlockSpec(memory_space=pl.ANY)] * len(before)
    return pl.pallas_call(
        finish_kernel,
        grid=(width // tile,),
        in_specs=given + held,
        out_specs=[
            whole,
            whole,
            whole,
            pl.BlockSpec((width // BLOCK, size), lambda k: (0, part)),
        ],
        out_shape=[jax.ShapeDtypeStruct(master.shape, jnp.float32)] * 3
        + [jax.ShapeDtypeStruct((width // BLOCK, rows), jnp.float32)],
        input_output_aliases={len(given) + k: k for k in range(len(before))},
    )(signs, table, kept, own, first, second, master, moment, variance, *before)


def gather_tokens(lows, highs, outer):
    parts = len(lows)
    if outer != 4:
        every = []
        for which, pieces in enumerate((lows, highs)):
            for part, piece in enumerate(pieces):
                whole = lax.all_gather(piece, "outer", axis=0, tiled=False)
                every += [(whole[k], which, part, k) for k in range(outer)]
        return every, None
    me = lax.axis_index("outer")
    even = (me == 0) | (me == 3)

    def across(value, distance):
        return lax.ppermute(value, "outer", [(k, k ^ distance) for k in range(outer)])

    near, far, corner = me ^ 1, me ^ 2, me ^ 3
    near_low = [across(lows[k], 1) for k in range(parts)]
    far_high = [across(highs[k], 2) for k in range(parts)]
    second_near = [across(jnp.where(even, highs[k], far_high[k]), 1) for k in range(parts)]
    second_far = [across(jnp.where(even, lows[k], near_low[k]), 2) for k in range(parts)]
    all_of = [jnp.concatenate(pieces, axis=1) for pieces in (lows, highs, near_low, far_high)]
    third_near = across(jnp.where(even, all_of[3], all_of[1]), 1)
    third_far = across(jnp.where(even, all_of[2], all_of[0]), 2)

    def end_block(owner, part):
        one = jnp.where(
            owner == me,
            lows[part],
            jnp.where(owner == near, near_low[part], second_far[part]),
        )
        two = jnp.where(
            owner == me,
            highs[part],
            jnp.where(owner == far, far_high[part], second_near[part]),
        )
        return one, two

    every = []
    for k in range(parts):
        every += [
            (lows[k], 0, k, me),
            (highs[k], 1, k, me),
            (near_low[k], 0, k, near),
            (far_high[k], 1, k, far),
            (second_near[k], 1, k, jnp.where(even, corner, near)),
            (second_far[k], 0, k, jnp.where(even, corner, far)),
        ]
    every += [
        (third_near, 1, 0, jnp.where(even, near, corner)),
        (third_far, 0, 0, jnp.where(even, far, corner)),
    ]
    return every, end_block


def contract(left, right):
    return lax.dot_general(
        left, right, (((0,), (0,)), ((), ())), preferred_element_type=jnp.float32
    )


def make_body(outer, inner):
    chips = inner // 2
    swap_pairs = [(k, k ^ 1) for k in range(inner)]
    up, down = [], []
    for z in range(chips - 1):
        up.append([(2 * z, 2 * z + 2), (2 * z + 1, 2 * z + 3)])
        down.append([(2 * z + 2, 2 * z), (2 * z + 3, 2 * z + 1)])
    top = 2 * chips - 2
    line_pairs = (
        [pair[0] for pair in up] + [pair[1] for pair in down] + [(top, top + 1), (1, 0)],
        [pair[1] for pair in up] + [pair[0] for pair in down] + [(top + 1, top), (0, 1)],
    )

    def swap(value):
        return lax.ppermute(value, "inner", swap_pairs)

    def along(line, value):
        return lax.ppermute(value, "inner", line_pairs[line])

    def body(tokens, cotangent, weight_cache, weight_delta, sign_bits, master, moment, variance):
        index = lax.axis_index("inner")
        chip, core = index // 2, index % 2
        rows, width = master.shape
        count, wide = tokens.shape
        group = wide // (2 * rows)
        signs = (1 - 2 * sign_bits).astype(jnp.float32)[None, :]
        table = sign_table(BLOCK).astype(jnp.bfloat16)
        upward = (core == 0, core == 1)

        def turned(line, position):
            return jnp.where(upward[line], position, chips - 1 - position)

        places = [turned(line, chip) for line in (0, 1)]

        parts = max(1, min(PARTS, rows // 128))
        size = rows // parts

        def columns_of(core_index, part):
            starts = [(2 * k + core_index) * rows + part * size for k in range(group)]
            return jnp.concatenate(
                [lax.dynamic_slice(tokens, (0, start), (count, size)) for start in starts],
                axis=1,
            )

        cut = [columns_of(which, part) for which in (core, 1 - core) for part in range(parts)]
        cut = lax.optimization_barrier(cut)
        lows = cut[:parts]
        highs = [swap(cut[parts + k]) for k in range(parts)]
        pieces, end_block = gather_tokens(lows, highs, outer)
        if chips != outer:
            end_block = None
        kept = [jnp.where(place == 0, 0.0, 1.0) for place in places]
        kept = jnp.stack(kept).astype(jnp.float32).reshape(1, 2)
        cotangent_other = swap(cotangent)
        held = jnp.zeros((outer, 2 * count, group, rows), tokens.dtype)
        for piece, which, part, owner in pieces:
            piece = piece.reshape(1, count, group, -1)
            held = lax.dynamic_update_slice(
                held, piece, (owner, which * count, 0, part * size)
            )
        held = held.reshape(outer, 2 * count, group * rows)

        def tokens_for(chip_index, which):
            column = lax.rem(chip_index, group) * rows
            return lax.dynamic_slice(
                held, (chip_index // group, which * count, column), (1, count, rows)
            )[0]

        def partial_sum(chip_index):
            one, two = tokens_for(chip_index, 0), tokens_for(chip_index, 1)
            return contract(one, cotangent) + contract(two, cotangent_other)

        def products(chip_index, deltas, cache):
            weights = []
            height = rows // len(deltas)
            for part, delta in enumerate(deltas):
                first = (2 * chip_index + core) * rows + part * height
                cached = lax.dynamic_slice(cache, (first, 0), (height, width))
                weight = cached.astype(jnp.float32) + delta.astype(jnp.float32)
                weights.append(lax.optimization_barrier(weight.astype(jnp.bfloat16)))
            return [
                [
                    jnp.dot(
                        tokens_for(chip_index, which)[:, part * height :][:, :height],
                        weight,
                        preferred_element_type=jnp.float32,
                    )
                    for part, weight in enumerate(weights)
                ]
                for which in (0, 1)
            ]

        halves = [weight_delta[k * size : (k + 1) * size] for k in range(parts)]
        message = [halves, halves]
        history = ([], [])
        cache = weight_cache
        caches = [cache]
        for turn in range(1, chips):
            terms = []
            for line in (0, 1):
                history[line].append([along(line, value) for value in message[line]])
                if turn > 1 or end_block is None:
                    target = turned(line, lax.rem(places[line] - turn + chips, chips))
                    term = partial_sum(target)
                    term = jnp.where(turn <= places[line], jnp.float32(0), term)
                    terms.append(lax.optimization_barrier(term))
            if turn == min(2, chips - 1):
                own = lax.optimization_barrier(partial_sum(chip))
            message = [[], []]
            for k in range(parts):
                rows_of = slice(k * size, (k + 1) * size)
                for line in (0, 1):
                    received, place = history[line][-1], places[line]
                    if terms:
                        term = terms[line][rows_of]
                    else:
                        one, two = end_block(turned(line, chips - 1), k)
                        term = contract(one, cotangent) + contract(two, cotangent_other)
                        term = jnp.where(turn <= place, jnp.float32(0), term)
                    before = jnp.where(place == 0, jnp.bfloat16(0), received[k])
                    value = (before.astype(jnp.float32) + term).astype(jnp.bfloat16)
                    cache, value, cotangent_other, *terms = lax.optimization_barrier(
                        (cache, value, cotangent_other, *terms)
                    )
                    message[line].append(value)
            caches.append(cache)

        last = [[along(line, message[line][k]) for line in (0, 1)] for k in range(parts)]
        mine, other = products(chip, [weight_delta], caches[1])
        mine, other = mine[0], other[0]
        order = sorted(range(1, chips), key=lambda t: max(t, chips - t))
        later = []
        for number, turn in enumerate(order, 1):
            passed = [history[0][turn - 1], history[1][chips - turn - 1]]
            deltas = [jnp.where(turn <= places[0], one, two) for one, two in zip(*passed)]
            source = turned(0, lax.rem(places[0] - turn + chips, chips))
            ones, twos = products(source, deltas, caches[max(turn, chips - turn)])
            for two in twos:
                other = other + two
            later.append((number, ones))
        theirs = swap(other)
        for number, ones in later:
            for k, one in enumerate(ones):
                mine = lax.optimization_barrier(mine)
                if number == chips - 1 and k == len(ones) - 1:
                    mine = mine + theirs
                mine = mine + one
        output = mine

        done = []
        for k in range(parts):
            done = finish(
                k, parts, signs, table, kept, own, *last[k], master, moment, variance, done
            )
        new_master, new_moment, new_variance, scales = done
        return (output, new_master, new_moment, new_variance, scales.T)

    return body


def solution(mesh):
    placed = (
        P("inner", "outer"),
        P("inner", "outer"),
        P(None, "outer"),
        P("inner", "outer"),
        P("outer"),
        P("inner", "outer"),
        P("inner", "outer"),
        P("inner", "outer"),
    )
    return jax.shard_map(
        make_body(mesh.shape["outer"], mesh.shape["inner"]),
        mesh=mesh,
        in_specs=placed,
        out_specs=(
            P("inner", "outer"),
            P("inner", "outer"),
            P("inner", "outer"),
            P("inner", "outer"),
            P("inner", "outer"),
        ),
        check_vma=False,
    )
```

```python
import functools

import jax
import jax.numpy as jnp
from jax import lax
from jax.experimental import pallas as pl
from jax.experimental.pallas import tpu as pltpu
from jax.sharding import PartitionSpec as P


BLOCK = 128
PARTS = 2


def sign_table(length):
    first = jnp.arange(length, dtype=jnp.int32)[:, None]
    second = jnp.arange(length, dtype=jnp.int32)[None, :]
    common = jnp.bitwise_and(first, second)
    parity = jnp.zeros((length, length), jnp.int32)
    for place in range(length.bit_length() - 1):
        parity = parity + jnp.bitwise_and(jnp.right_shift(common, place), 1)
    return 1 - 2 * (parity % 2)


def finish_kernel(start, signs, table, kept, own, first, second, master, moment, variance, *rest):
    new_master, new_moment, new_variance, scales = rest[-4:]
    tile = new_master.shape[0]
    near = pl.ds(pl.multiple_of(pl.program_id(0) * tile, tile), tile)
    far = pl.ds(pl.multiple_of(start + pl.program_id(0) * tile, tile), tile)
    gradient = own[far, :]
    for line, received in enumerate((first, second)):
        wanted = kept[:, line : line + 1] > 0.0
        gradient = gradient + jnp.where(wanted, received[near, :].astype(jnp.float32), 0.0)
    first_moment = 0.9 * moment[far, :] + 0.1 * gradient
    second_moment = 0.95 * variance[far, :] + 0.05 * gradient * gradient
    corrected = first_moment / (1.0 - 0.9**10)
    spread = jnp.sqrt(second_moment / (1.0 - 0.95**10)) + 1e-08
    new_moment[...] = first_moment
    new_variance[...] = second_moment
    given = master[far, :]
    new_master[...] = given - 0.01 * (corrected / spread + 0.1 * given)
    for place in range(gradient.shape[1] // BLOCK):
        columns = slice(place * BLOCK, (place + 1) * BLOCK)
        signed = gradient[:, columns] * signs[:, columns]
        high = signed.astype(jnp.bfloat16)
        low = (signed - high.astype(jnp.float32)).astype(jnp.bfloat16)
        mixed = sum(
            lax.dot_general(
                table[...], term, (((1,), (1,)), ((), ())), preferred_element_type=jnp.float32
            )
            for term in (high, low)
        )
        largest = jnp.max(jnp.abs(mixed), axis=0, keepdims=True)
        scales[place : place + 1, :] = largest * (1.0 / BLOCK**0.5)


def finish(start, given, before):
    rows, width = given[-1].shape
    size = given[4].shape[0]
    tile = min(size, 128)
    first = start // tile
    whole = pl.BlockSpec((tile, width), lambda k: (first + k, 0))
    given = [pltpu.with_memory_space_constraint(value, pltpu.VMEM) for value in given]
    return pl.pallas_call(
        functools.partial(finish_kernel, start),
        grid=(size // tile,),
        in_specs=[pl.BlockSpec(memory_space=pltpu.VMEM)] * len(given)
        + [pl.BlockSpec(memory_space=pl.ANY)] * len(before),
        out_specs=[
            whole,
            whole,
            whole,
            pl.BlockSpec((width // BLOCK, tile), lambda k: (0, first + k)),
        ],
        out_shape=[jax.ShapeDtypeStruct((rows, width), jnp.float32)] * 3
        + [jax.ShapeDtypeStruct((width // BLOCK, rows), jnp.float32)],
        input_output_aliases={len(given) + k: k for k in range(len(before))},
        compiler_params=pltpu.CompilerParams(vmem_limit_bytes=16 * tile * width * 4),
    )(*given, *before)


def gather_tokens(lows, highs, outer, inner):
    parts = len(lows)
    if outer != 4:
        every = []
        for which, pieces in enumerate((lows, highs)):
            for part, piece in enumerate(pieces):
                whole = lax.all_gather(piece, "outer", axis=0, tiled=False)
                every += [(whole[k], which, part, k) for k in range(outer)]
        return every, None
    me = lax.axis_index("outer")
    core = lax.axis_index("inner") % 2
    even = (me == 0) | (me == 3)
    distances = ((1, 2), (2, 1))

    def across(value, turn):
        pairs = []
        for place in range(outer):
            for index in range(inner):
                other = place ^ distances[index % 2][turn]
                pairs.append((place * inner + index, other * inner + index))
        return lax.ppermute(value, ("outer", "inner"), pairs)

    one = me ^ jnp.where(core == 0, 1, 2)
    two = me ^ jnp.where(core == 0, 2, 1)
    corner = me ^ 3
    low_of_one = [across(lows[k], 0) for k in range(parts)]
    high_of_two = [across(highs[k], 1) for k in range(parts)]
    second_low = [across(jnp.where(even, lows[k], low_of_one[k]), 1) for k in range(parts)]
    second_high = [across(jnp.where(even, highs[k], high_of_two[k]), 0) for k in range(parts)]
    every = [jnp.concatenate(pieces, axis=1) for pieces in (lows, highs, low_of_one, high_of_two)]
    third_low = across(jnp.where(even, every[2], every[0]), 1)
    third_high = across(jnp.where(even, every[3], every[1]), 0)

    def end_block(owner, part):
        low = jnp.where(owner == one, low_of_one[part], second_low[part])
        high = jnp.where(owner == two, high_of_two[part], second_high[part])
        return (
            jnp.where(owner == me, lows[part], low),
            jnp.where(owner == me, highs[part], high),
        )

    every = []
    for k in range(parts):
        every += [
            (lows[k], 0, k, me),
            (highs[k], 1, k, me),
            (low_of_one[k], 0, k, one),
            (high_of_two[k], 1, k, two),
            (second_high[k], 1, k, jnp.where(even, corner, one)),
            (second_low[k], 0, k, jnp.where(even, corner, two)),
        ]
    every += [
        (third_high, 1, 0, jnp.where(even, one, corner)),
        (third_low, 0, 0, jnp.where(even, two, corner)),
    ]
    return every, end_block


def contract(left, right):
    return lax.dot_general(
        left, right, (((0,), (0,)), ((), ())), preferred_element_type=jnp.float32
    )


def make_body(outer, inner):
    chips = inner // 2
    swap_pairs = [(k, k ^ 1) for k in range(inner)]
    up, down = [], []
    for z in range(chips - 1):
        up.append([(2 * z, 2 * z + 2), (2 * z + 1, 2 * z + 3)])
        down.append([(2 * z + 2, 2 * z), (2 * z + 3, 2 * z + 1)])
    top = 2 * chips - 2
    line_pairs = (
        [pair[0] for pair in up] + [pair[1] for pair in down] + [(top, top + 1), (1, 0)],
        [pair[1] for pair in up] + [pair[0] for pair in down] + [(top + 1, top), (0, 1)],
    )

    def swap(value):
        return lax.ppermute(value, "inner", swap_pairs)

    def along(line, value):
        return lax.ppermute(value, "inner", line_pairs[line])

    def body(tokens, cotangent, weight_cache, weight_delta, sign_bits, master, moment, variance):
        index = lax.axis_index("inner")
        chip, core = index // 2, index % 2
        rows, width = master.shape
        count, wide = tokens.shape
        group = wide // (2 * rows)
        signs = (1 - 2 * sign_bits).astype(jnp.float32)[None, :]
        table = sign_table(BLOCK).astype(jnp.bfloat16)
        upward = (core == 0, core == 1)

        def turned(line, position):
            return jnp.where(upward[line], position, chips - 1 - position)

        places = [turned(line, chip) for line in (0, 1)]

        parts = max(1, min(PARTS, rows // 128))
        size = rows // parts

        def columns_of(core_index, part):
            starts = [(2 * k + core_index) * rows + part * size for k in range(group)]
            return jnp.concatenate(
                [lax.dynamic_slice(tokens, (0, start), (count, size)) for start in starts],
                axis=1,
            )

        lows, highs = [], []
        for part in range(parts):
            low, high = lax.optimization_barrier(
                (columns_of(core, part), columns_of(1 - core, part))
            )
            lows.append(low)
            highs.append(swap(high))
        pieces, end_block = gather_tokens(lows, highs, outer, inner)
        if chips != outer:
            end_block = None
        kept = [jnp.where(place == 0, 0.0, 1.0) for place in places]
        kept = jnp.stack(kept).astype(jnp.float32).reshape(1, 2)
        cotangent_other = swap(cotangent)
        held = jnp.zeros((outer, 2 * count, group, rows), tokens.dtype)
        for piece, which, part, owner in pieces:
            piece = piece.reshape(1, count, group, -1)
            held = lax.dynamic_update_slice(
                held, piece, (owner, which * count, 0, part * size)
            )
        held = held.reshape(outer, 2 * count, group * rows)

        def tokens_for(chip_index, which):
            column = lax.rem(chip_index, group) * rows
            return lax.dynamic_slice(
                held, (chip_index // group, which * count, column), (1, count, rows)
            )[0]

        def partial_sum(chip_index):
            one, two = tokens_for(chip_index, 0), tokens_for(chip_index, 1)
            return contract(one, cotangent) + contract(two, cotangent_other)

        def products(chip_index, deltas, cache):
            weights = []
            height = rows // len(deltas)
            for part, delta in enumerate(deltas):
                first = (2 * chip_index + core) * rows + part * height
                cached = lax.dynamic_slice(cache, (first, 0), (height, width))
                weight = cached.astype(jnp.float32) + delta.astype(jnp.float32)
                weights.append(lax.optimization_barrier(weight.astype(jnp.bfloat16)))
            return [
                [
                    jnp.dot(
                        tokens_for(chip_index, which)[:, part * height :][:, :height],
                        weight,
                        preferred_element_type=jnp.float32,
                    )
                    for part, weight in enumerate(weights)
                ]
                for which in (0, 1)
            ]

        def pieces_of(turn):
            found = [(k, 0, size) for k in range(parts)]
            if turn == chips and size % 256 == 0:
                half = size // 2
                found[-1:] = [(parts - 1, 0, half), (parts - 1, half, half)]
            return found

        message = [[weight_delta], [weight_delta]]
        history = ([], [])
        cache = weight_cache
        caches = [cache]
        for turn in range(1, chips):
            terms = []
            for line in (0, 1):
                history[line].append([along(line, value) for value in message[line]])
                if turn > 1 or end_block is None:
                    target = turned(line, lax.rem(places[line] - turn + chips, chips))
                    term = partial_sum(target)
                    term = jnp.where(turn <= places[line], jnp.float32(0), term)
                    terms.append(lax.optimization_barrier(term))
            if turn == min(2, chips - 1):
                own = lax.optimization_barrier(partial_sum(chip))
            message = [[], []]
            for k, offset, height in pieces_of(turn + 1):
                rows_of = slice(k * size + offset, k * size + offset + height)
                inside = slice(offset, offset + height)
                for line in (0, 1):
                    received, place = history[line][-1], places[line]
                    if terms:
                        term = terms[line][rows_of]
                    else:
                        one, two = end_block(turned(line, chips - 1), k)
                        term = contract(one[:, inside], cotangent)
                        term = term + contract(two[:, inside], cotangent_other)
                        term = jnp.where(turn <= place, jnp.float32(0), term)
                    whole = len(received) == 1
                    before = received[0][rows_of] if whole else received[k][inside]
                    before = jnp.where(place == 0, jnp.bfloat16(0), before)
                    value = (before.astype(jnp.float32) + term).astype(jnp.bfloat16)
                    cache, value, cotangent_other, *terms = lax.optimization_barrier(
                        (cache, value, cotangent_other, *terms)
                    )
                    message[line].append(value)
            caches.append(cache)

        last = [[along(line, message[line][k]) for line in (0, 1)] for k in range(len(message[0]))]

        def cut(values):
            if len(values) == parts:
                return values
            return [values[0][k * size : (k + 1) * size] for k in range(parts)]

        mine, other = products(chip, [weight_delta], caches[1])
        mine, other = mine[0], other[0]
        order = sorted(range(1, chips), key=lambda t: max(t, chips - t))
        later = []
        for number, turn in enumerate(order, 1):
            passed = [cut(history[0][turn - 1]), cut(history[1][chips - turn - 1])]
            deltas = [jnp.where(turn <= places[0], one, two) for one, two in zip(*passed)]
            source = turned(0, lax.rem(places[0] - turn + chips, chips))
            ones, twos = products(source, deltas, caches[max(turn, chips - turn)])
            for two in twos:
                other = other + two
            later.append((number, ones))
        theirs = swap(other)
        for number, ones in later:
            for k, one in enumerate(ones):
                mine = lax.optimization_barrier(mine)
                if number == chips - 1 and k == len(ones) - 1:
                    mine = mine + theirs
                mine = mine + one
        output = mine

        done = []
        for number, (k, offset, _) in enumerate(pieces_of(chips)):
            given = [signs, table, kept, own, *last[number], master, moment, variance]
            done = finish(k * size + offset, given, done)
        new_master, new_moment, new_variance, scales = done
        return (output, new_master, new_moment, new_variance, scales.T)

    return body


def solution(mesh):
    placed = (
        P("inner", "outer"),
        P("inner", "outer"),
        P(None, "outer"),
        P("inner", "outer"),
        P("outer"),
        P("inner", "outer"),
        P("inner", "outer"),
        P("inner", "outer"),
    )
    return jax.shard_map(
        make_body(mesh.shape["outer"], mesh.shape["inner"]),
        mesh=mesh,
        in_specs=placed,
        out_specs=(
            P("inner", "outer"),
            P("inner", "outer"),
            P("inner", "outer"),
            P("inner", "outer"),
            P("inner", "outer"),
        ),
        check_vma=False,
    )
```

```python
import functools

import jax
import jax.numpy as jnp
from jax import lax
from jax.experimental import pallas as pl
from jax.experimental.pallas import tpu as pltpu
from jax.sharding import PartitionSpec as P


BLOCK = 128
PARTS = 2


def sign_table(length):
    first = jnp.arange(length, dtype=jnp.int32)[:, None]
    second = jnp.arange(length, dtype=jnp.int32)[None, :]
    common = jnp.bitwise_and(first, second)
    parity = jnp.zeros((length, length), jnp.int32)
    for place in range(length.bit_length() - 1):
        parity = parity + jnp.bitwise_and(jnp.right_shift(common, place), 1)
    return 1 - 2 * (parity % 2)


def finish_kernel(start, signs, table, kept, own, first, second, master, moment, variance, *rest):
    new_master, new_moment, new_variance, scales = rest[-4:]
    tile = new_master.shape[0]
    near = pl.ds(pl.multiple_of(pl.program_id(0) * tile, tile), tile)
    far = pl.ds(pl.multiple_of(start + pl.program_id(0) * tile, tile), tile)
    gradient = own[far, :]
    for line, received in enumerate((first, second)):
        wanted = kept[:, line : line + 1] > 0.0
        gradient = gradient + jnp.where(wanted, received[near, :].astype(jnp.float32), 0.0)
    first_moment = 0.9 * moment[far, :] + 0.1 * gradient
    second_moment = 0.95 * variance[far, :] + 0.05 * gradient * gradient
    corrected = first_moment / (1.0 - 0.9**10)
    spread = jnp.sqrt(second_moment / (1.0 - 0.95**10)) + 1e-08
    new_moment[...] = first_moment
    new_variance[...] = second_moment
    given = master[far, :]
    new_master[...] = given - 0.01 * (corrected / spread + 0.1 * given)
    for place in range(gradient.shape[1] // BLOCK):
        columns = slice(place * BLOCK, (place + 1) * BLOCK)
        signed = gradient[:, columns] * signs[:, columns]
        high = signed.astype(jnp.bfloat16)
        low = (signed - high.astype(jnp.float32)).astype(jnp.bfloat16)
        mixed = sum(
            lax.dot_general(
                table[...], term, (((1,), (1,)), ((), ())), preferred_element_type=jnp.float32
            )
            for term in (high, low)
        )
        largest = jnp.max(jnp.abs(mixed), axis=0, keepdims=True)
        scales[place : place + 1, :] = largest * (1.0 / BLOCK**0.5)


def finish(start, given, before):
    rows, width = given[-1].shape
    size = given[4].shape[0]
    tile = min(size, 128)
    first = start // tile
    whole = pl.BlockSpec((tile, width), lambda k: (first + k, 0))
    given = [pltpu.with_memory_space_constraint(value, pltpu.VMEM) for value in given]
    return pl.pallas_call(
        functools.partial(finish_kernel, start),
        grid=(size // tile,),
        in_specs=[pl.BlockSpec(memory_space=pltpu.VMEM)] * len(given)
        + [pl.BlockSpec(memory_space=pl.ANY)] * len(before),
        out_specs=[
            whole,
            whole,
            whole,
            pl.BlockSpec((width // BLOCK, tile), lambda k: (0, first + k)),
        ],
        out_shape=[jax.ShapeDtypeStruct((rows, width), jnp.float32)] * 3
        + [jax.ShapeDtypeStruct((width // BLOCK, rows), jnp.float32)],
        input_output_aliases={len(given) + k: k for k in range(len(before))},
        compiler_params=pltpu.CompilerParams(vmem_limit_bytes=16 * tile * width * 4),
    )(*given, *before)


def gather_tokens(lows, highs, outer, inner):
    parts = len(lows)
    if outer != 4:
        every = []
        for which, pieces in enumerate((lows, highs)):
            for part, piece in enumerate(pieces):
                whole = lax.all_gather(piece, "outer", axis=0, tiled=False)
                every += [(whole[k], which, part, k) for k in range(outer)]
        return every, None
    me = lax.axis_index("outer")
    core = lax.axis_index("inner") % 2
    even = (me == 0) | (me == 3)
    distances = ((1, 2), (2, 1))

    def across(value, turn):
        pairs = []
        for place in range(outer):
            for index in range(inner):
                other = place ^ distances[index % 2][turn]
                pairs.append((place * inner + index, other * inner + index))
        return lax.ppermute(value, ("outer", "inner"), pairs)

    one = me ^ jnp.where(core == 0, 1, 2)
    two = me ^ jnp.where(core == 0, 2, 1)
    corner = me ^ 3
    low_of_one = [across(lows[k], 0) for k in range(parts)]
    high_of_two = [across(highs[k], 1) for k in range(parts)]
    second_low = [across(jnp.where(even, lows[k], low_of_one[k]), 1) for k in range(parts)]
    second_high = [across(jnp.where(even, highs[k], high_of_two[k]), 0) for k in range(parts)]
    every = [jnp.concatenate(pieces, axis=1) for pieces in (lows, highs, low_of_one, high_of_two)]
    third_low = across(jnp.where(even, every[2], every[0]), 1)
    third_high = across(jnp.where(even, every[3], every[1]), 0)

    def end_block(owner, part):
        low = jnp.where(owner == one, low_of_one[part], second_low[part])
        high = jnp.where(owner == two, high_of_two[part], second_high[part])
        return (
            jnp.where(owner == me, lows[part], low),
            jnp.where(owner == me, highs[part], high),
        )

    every = []
    for k in range(parts):
        every += [
            (lows[k], 0, k, me),
            (highs[k], 1, k, me),
            (low_of_one[k], 0, k, one),
            (high_of_two[k], 1, k, two),
            (second_high[k], 1, k, jnp.where(even, corner, one)),
            (second_low[k], 0, k, jnp.where(even, corner, two)),
        ]
    every += [
        (third_high, 1, 0, jnp.where(even, one, corner)),
        (third_low, 0, 0, jnp.where(even, two, corner)),
    ]
    return every, end_block


def contract(left, right):
    return lax.dot_general(
        left, right, (((0,), (0,)), ((), ())), preferred_element_type=jnp.float32
    )


def make_body(outer, inner):
    chips = inner // 2
    swap_pairs = [(k, k ^ 1) for k in range(inner)]
    up, down = [], []
    for z in range(chips - 1):
        up.append([(2 * z, 2 * z + 2), (2 * z + 1, 2 * z + 3)])
        down.append([(2 * z + 2, 2 * z), (2 * z + 3, 2 * z + 1)])
    top = 2 * chips - 2
    line_pairs = (
        [pair[0] for pair in up] + [pair[1] for pair in down] + [(top, top + 1), (1, 0)],
        [pair[1] for pair in up] + [pair[0] for pair in down] + [(top + 1, top), (0, 1)],
    )

    def swap(value):
        return lax.ppermute(value, "inner", swap_pairs)

    def along(line, value):
        return lax.ppermute(value, "inner", line_pairs[line])

    def body(tokens, cotangent, weight_cache, weight_delta, sign_bits, master, moment, variance):
        index = lax.axis_index("inner")
        chip, core = index // 2, index % 2
        rows, width = master.shape
        count, wide = tokens.shape
        group = wide // (2 * rows)
        signs = (1 - 2 * sign_bits).astype(jnp.float32)[None, :]
        table = sign_table(BLOCK).astype(jnp.bfloat16)
        upward = (core == 0, core == 1)

        def turned(line, position):
            return jnp.where(upward[line], position, chips - 1 - position)

        places = [turned(line, chip) for line in (0, 1)]

        parts = max(1, min(PARTS, rows // 128))
        size = rows // parts

        def columns_of(core_index, part):
            starts = [(2 * k + core_index) * rows + part * size for k in range(group)]
            return jnp.concatenate(
                [lax.dynamic_slice(tokens, (0, start), (count, size)) for start in starts],
                axis=1,
            )

        lows, highs = [], []
        for part in range(parts):
            low, high = lax.optimization_barrier(
                (columns_of(core, part), columns_of(1 - core, part))
            )
            lows.append(low)
            highs.append(swap(high))
        pieces, end_block = gather_tokens(lows, highs, outer, inner)
        if chips != outer:
            end_block = None
        kept = [jnp.where(place == 0, 0.0, 1.0) for place in places]
        kept = jnp.stack(kept).astype(jnp.float32).reshape(1, 2)
        cotangent_other = swap(cotangent)
        held = jnp.zeros((outer, 2 * count, group, rows), tokens.dtype)
        for piece, which, part, owner in pieces:
            piece = piece.reshape(1, count, group, -1)
            held = lax.dynamic_update_slice(
                held, piece, (owner, which * count, 0, part * size)
            )
        held = held.reshape(outer, 2 * count, group * rows)

        def tokens_for(chip_index, which):
            column = lax.rem(chip_index, group) * rows
            return lax.dynamic_slice(
                held, (chip_index // group, which * count, column), (1, count, rows)
            )[0]

        def partial_sum(chip_index):
            one, two = tokens_for(chip_index, 0), tokens_for(chip_index, 1)
            return contract(one, cotangent) + contract(two, cotangent_other)

        def products(chip_index, deltas, cache):
            weights = []
            height = rows // len(deltas)
            for part, delta in enumerate(deltas):
                first = (2 * chip_index + core) * rows + part * height
                cached = lax.dynamic_slice(cache, (first, 0), (height, width))
                weight = cached.astype(jnp.float32) + delta.astype(jnp.float32)
                weights.append(lax.optimization_barrier(weight.astype(jnp.bfloat16)))
            found = [[], []]
            for which in (0, 1):
                for part, weight in enumerate(weights):
                    given = tokens_for(chip_index, which)[:, part * height :][:, :height]
                    found[which].append(jnp.dot(given, weight, preferred_element_type=jnp.float32))
            return found

        def pieces_of(turn):
            found = [(k, 0, size) for k in range(parts)]
            if turn == chips and size % 256 == 0:
                half = size // 2
                found[-1:] = [(parts - 1, 0, half), (parts - 1, half, half)]
            return found

        message = [[weight_delta], [weight_delta]]
        history = ([], [])
        cache = weight_cache
        caches = [cache]
        for turn in range(1, chips):
            terms = []
            for line in (0, 1):
                history[line].append([along(line, value) for value in message[line]])
                if turn > 1 or end_block is None:
                    target = turned(line, lax.rem(places[line] - turn + chips, chips))
                    term = partial_sum(target)
                    term = jnp.where(turn <= places[line], jnp.float32(0), term)
                    terms.append(lax.optimization_barrier(term))
            if turn == min(2, chips - 1):
                own = lax.optimization_barrier(partial_sum(chip))
            message = [[], []]
            for k, offset, height in pieces_of(turn + 1):
                rows_of = slice(k * size + offset, k * size + offset + height)
                inside = slice(offset, offset + height)
                for line in (0, 1):
                    received, place = history[line][-1], places[line]
                    if terms:
                        term = terms[line][rows_of]
                    else:
                        one, two = end_block(turned(line, chips - 1), k)
                        term = contract(one[:, inside], cotangent)
                        term = term + contract(two[:, inside], cotangent_other)
                        term = jnp.where(turn <= place, jnp.float32(0), term)
                    whole = len(received) == 1
                    before = received[0][rows_of] if whole else received[k][inside]
                    before = jnp.where(place == 0, jnp.bfloat16(0), before)
                    value = (before.astype(jnp.float32) + term).astype(jnp.bfloat16)
                    cache, value, cotangent_other, *terms = lax.optimization_barrier(
                        (cache, value, cotangent_other, *terms)
                    )
                    message[line].append(value)
            caches.append(cache)

        last = [[along(line, message[line][k]) for line in (0, 1)] for k in range(len(message[0]))]

        def cut(values):
            if len(values) == parts:
                return values
            return [values[0][k * size : (k + 1) * size] for k in range(parts)]

        mine, other = products(chip, [weight_delta], caches[1])
        mine, other = mine[0], other[0]
        for line in (0, 1):
            history[line][0] = [
                lax.optimization_barrier(jnp.where(places[line] == 0, jnp.bfloat16(0), value))
                for value in history[line][0]
            ]
        order = sorted(range(1, chips), key=lambda t: max(t, chips - t))
        later = []
        for number, turn in enumerate(order, 1):
            passed = [cut(history[0][turn - 1]), cut(history[1][chips - turn - 1])]
            deltas = [jnp.where(turn <= places[0], one, two) for one, two in zip(*passed)]
            source = turned(0, lax.rem(places[0] - turn + chips, chips))
            ones, twos = products(source, deltas, caches[max(turn, chips - turn)])
            for two in twos:
                other = other + two
            later.append((number, ones))
        theirs = swap(other)
        for number, ones in later:
            for k, one in enumerate(ones):
                mine = lax.optimization_barrier(mine)
                if number == chips - 1 and k == len(ones) - 1:
                    mine = mine + theirs
                mine = mine + one
        output = mine

        done = []
        for number, (k, offset, _) in enumerate(pieces_of(chips)):
            given = [signs, table, kept, own, *last[number], master, moment, variance]
            done = finish(k * size + offset, given, done)
        new_master, new_moment, new_variance, scales = done
        return (output, new_master, new_moment, new_variance, scales.T)

    return body


def solution(mesh):
    placed = (
        P("inner", "outer"),
        P("inner", "outer"),
        P(None, "outer"),
        P("inner", "outer"),
        P("outer"),
        P("inner", "outer"),
        P("inner", "outer"),
        P("inner", "outer"),
    )
    return jax.shard_map(
        make_body(mesh.shape["outer"], mesh.shape["inner"]),
        mesh=mesh,
        in_specs=placed,
        out_specs=(
            P("inner", "outer"),
            P("inner", "outer"),
            P("inner", "outer"),
            P("inner", "outer"),
            P("inner", "outer"),
        ),
        check_vma=False,
    )
```
